512 devices in a mesh: blk: 32 (over z_lo, x), col: 16 (over y, z_hi, core).
Axes of the slice: x: 4, y: 4, z: 16 (z_hi: 2, z_lo: 8; z = z_hi * 8 + z_lo), core: 2. Of those that a mesh axis runs over, the one named last changes fastest.
Arguments:
- old_vectors: float32 [1024, 262144], P('col', 'blk'), may hold values from -6 to 6
- merge_matrix: float32 [1024, 1024], P('col', 'blk'), may hold values from -0.1875 to 0.1875
- deflation_order: int32 [1024], P('col'), may hold values from 0 to 63, as said below
- kept_counts: int32 [16], P('col'), may hold values from 1 to 64
Outputs:
- new_vectors: float32 [2, 32, 262144], P(None, None, ('blk', 'col'))
The draws below stay inside these ranges and needn't reach their ends.
Inputs may be any that keep to these rules, and one draw needn't show every extreme that they name: `deflation_order`: each aligned block of 64 entries holds every number 0 to 63 once.
All inputs are finite; a program needn't handle non-finite values.
Results may differ from the reference program's by a relative error of at most 0.0001.
Values sent between devices are 32-bit elements; how exact they have to be, the bound alone decides.
No kernel may reach another device: no remote copies, remote signals or barrier semaphores. Data moves between devices by JAX's collectives and lax.ppermute only.
A program may use at most 64 MiB of HBM per device.

```python
import jax
import jax.numpy as jnp
from jax import lax

K = 1024
J = 1024
ROWS = 8192
STEPS = 2
N = 262144
KC = 64
JB = 32
N_BLK = 32


def draw_deflation_order(key, part):
    scores = jax.random.randint(jax.random.fold_in(key, 17), (K // KC, KC), 0, 2 ** 20)
    ranked = scores * KC + lax.broadcasted_iota(jnp.int32, (K // KC, KC), 1)
    return jnp.argsort(ranked, axis=1).astype(jnp.int32).reshape(K)


def plant(entries, rng, least, top_value):
    index_at = [jax.random.randint(jax.random.fold_in(rng, axis), (), 0, length) for axis, length in enumerate(entries.shape)]
    widest = entries.shape.index(max(entries.shape))
    neighbour = index_at[:widest] + [(index_at[widest] + 1) % entries.shape[widest]] + index_at[widest + 1:]
    return entries.at[tuple(index_at)].set(least).at[tuple(neighbour)].set(top_value)


def shard_levels(stream_key, dims, split, low, top_value):
    loudness = 1.0
    for axis_at, shards_of in split:
        draws = jax.random.uniform(jax.random.fold_in(jax.random.fold_in(stream_key, 6), axis_at), (shards_of,), jnp.float32, low / len(split), top_value / len(split))
        loudness = loudness * jnp.repeat(jnp.exp(draws), dims[axis_at] // shards_of).reshape((-1,) + (1,) * (len(dims) - 1 - axis_at))
    return loudness


def bell_draw(rng, dims, width, reach, shards=(), dtype=jnp.bfloat16):
    drawn = width * jax.random.normal(rng, dims, jnp.float32)
    if shards:
        drawn = drawn * shard_levels(rng, dims, shards, -0.22, 0.18)
    return jnp.clip(drawn, -reach, reach).astype(dtype)


def setup_inputs(seed: int = 0) -> dict:
    key_of = jax.random.split(jax.random.key(seed), 5)
    old_vectors = bell_draw(key_of[0], (K, N), 1.0, 6.0, ((0, 16), (1, 32)), jnp.float32)
    merge_matrix = bell_draw(key_of[1], (K, J), K ** -0.5, 0.1875, ((0, 16), (1, 32)), jnp.float32)
    deflation_order = draw_deflation_order(jax.random.fold_in(key_of[4], 71), 0)
    kept_counts = plant(jax.random.randint(key_of[3], (K // KC,), 1, KC + 1), jax.random.fold_in(key_of[3], 1), 1, KC).astype(jnp.int32)
    return {"old_vectors": old_vectors, "merge_matrix": merge_matrix, "deflation_order": deflation_order, "kept_counts": kept_counts}


def reference(old_vectors, merge_matrix, deflation_order, kept_counts):
    blocks_col = K // KC
    shaped = merge_matrix.reshape(blocks_col, KC, J)
    picked = jnp.take_along_axis(shaped, deflation_order.reshape(blocks_col, KC)[:, :, None].astype(jnp.int32), axis=1)
    position = lax.broadcasted_iota(jnp.int32, (blocks_col, KC, 1), 1)
    deflated = jnp.where(position < kept_counts[:, None, None], picked, jnp.float32(0.0)).reshape(K, J)
    slabs = jnp.transpose(deflated.reshape(K, N_BLK, JB), (1, 0, 2))
    row_blocks = jnp.transpose(old_vectors.reshape(K, N_BLK, ROWS), (1, 0, 2))
    results = []
    for turn_index in range(STEPS):
        rolled = jnp.roll(row_blocks, turn_index, axis=0)
        partial_out = jnp.einsum("bkr,bkj->bjr", rolled.astype(jnp.float32), slabs.astype(jnp.float32), precision=lax.Precision.HIGHEST)
        results.append(jnp.transpose(partial_out, (1, 0, 2)).reshape(JB, N))
    return jnp.stack(results)
```

```python
import functools

import jax
import jax.numpy as jnp
from jax import lax
from jax.experimental import pallas as pl
from jax.experimental.pallas import tpu as pltpu
from jax.sharding import Mesh, PartitionSpec as P

AXES = ("zl", "x", "y", "zh", "core")
SIZES = (8, 4, 4, 2, 2)
NBLK = 32


def prep_kernel(core_ref, kept_ref, order_ref, merge_ref, q_ref, ut_ref, send_ref, sem):
    other = 1 - core_ref[0]
    pieces = send_ref.shape[0]
    width = send_ref.shape[2]
    copies = []
    for g in range(pieces):
        start = pl.multiple_of((2 * g + other) * width, width)
        copies.append(pltpu.make_async_copy(q_ref.at[:, pl.ds(start, width)], send_ref.at[g], sem.at[g]))
    for c in copies:
        c.start()
    n = merge_ref.shape[0]
    rows = lax.broadcasted_iota(jnp.int32, (n, n), 0)
    place = lax.broadcasted_iota(jnp.int32, (n, n), 1)
    hit = (rows == order_ref[...]) & (place < kept_ref[0])
    ut_ref[...] = lax.dot_general(
        merge_ref[...],
        hit.astype(jnp.float32),
        (((0,), (0,)), ((), ())),
        precision=lax.Precision.HIGHEST,
        preferred_element_type=jnp.float32,
    )
    for c in copies:
        c.wait()


def prepare(core, kept, order, merge, q):
    k, j = merge.shape
    pieces, width = 8, q.shape[1] // 16
    return pl.pallas_call(
        prep_kernel,
        out_shape=(
            jax.ShapeDtypeStruct((j, k), jnp.float32),
            jax.ShapeDtypeStruct((pieces, k, width), jnp.float32),
        ),
        in_specs=[
            pl.BlockSpec(memory_space=pltpu.SMEM),
            pl.BlockSpec(memory_space=pltpu.SMEM),
            pl.BlockSpec(memory_space=pltpu.VMEM),
            pl.BlockSpec(memory_space=pltpu.VMEM),
            pl.BlockSpec(memory_space=pl.ANY),
        ],
        out_specs=(
            pl.BlockSpec(memory_space=pltpu.VMEM),
            pl.BlockSpec(memory_space=pl.ANY),
        ),
        scratch_shapes=[pltpu.SemaphoreType.DMA((pieces,))],
        name="prep",
    )(core, kept, order, merge, q)


def multiply_kernel(where_ref, ut_ref, q_ref, got_ref, out_ref):
    core, zh, flip = where_ref[0], where_ref[1], where_ref[2]
    g = pl.program_id(0)
    zt = g % 2
    j = ut_ref.shape[1] // 2
    u = jnp.concatenate([ut_ref[core], ut_ref[1 - core]], axis=1)
    qq = jnp.concatenate([q_ref[...], got_ref[0]], axis=0)
    prod = lax.dot_general(
        u,
        qq,
        (((1,), (0,)), ((), ())),
        precision=lax.Precision.HIGHEST,
        preferred_element_type=jnp.float32,
    )
    late0 = (zt == zh).astype(jnp.int32)
    late1 = (late0 + flip) % 2
    out_ref[late0, g // 2, 0:j, :] = prod[0:j]
    out_ref[late1, g // 2, j : 2 * j, :] = prod[j : 2 * j]


def multiply(where, ut, q, got):
    pieces, k, width = got.shape
    rows = ut.shape[1]
    return pl.pallas_call(
        multiply_kernel,
        grid_spec=pltpu.PrefetchScalarGridSpec(
            num_scalar_prefetch=1,
            grid=(pieces,),
            in_specs=[
                pl.BlockSpec(ut.shape, lambda g, w: (0, 0, 0)),
                pl.BlockSpec((k, width), lambda g, w: (0, 2 * g + w[0])),
                pl.BlockSpec((1, k, width), lambda g, w: (g, 0, 0)),
            ],
            out_specs=pl.BlockSpec((2, pieces // 2, rows, width), lambda g, w: (0, 0, 0, 0)),
        ),
        out_shape=jax.ShapeDtypeStruct((2, pieces // 2, rows, width), jnp.float32),
        name="multiply",
    )(where, ut, q, got)


def pairs_of(move):
    pairs = []
    for b in range(NBLK):
        for zh in range(2):
            tb, tz = move(b, zh)
            pairs.append((b * 2 + zh, tb * 2 + tz))
    return pairs


BACK = pairs_of(lambda b, zh: ((b - 1) % NBLK, zh))
AHEAD = pairs_of(lambda b, zh: ((b + 1) % NBLK, zh if b < NBLK - 1 else 1 - zh))
SWAP = [(0, 1), (1, 0)]
ROUND = ("zl", "x", "zh")


def shards(old_vectors, merge_matrix, deflation_order, kept_counts):
    core = lax.axis_index("core").astype(jnp.int32)
    zh = lax.axis_index("zh").astype(jnp.int32)
    last = (lax.axis_index(("zl", "x")) == NBLK - 1).astype(jnp.int32)
    k, j = merge_matrix.shape
    ut, send = prepare(core.reshape(1), kept_counts, deflation_order.reshape(1, k), merge_matrix, old_vectors)
    ut_next = lax.ppermute(ut, ROUND, BACK)
    got = lax.ppermute(send, "core", SWAP)
    both = lax.all_gather(jnp.concatenate([ut, ut_next], axis=0), "core")
    parts = multiply(jnp.stack([core, zh, last]), both, old_vectors, got)
    early = lax.all_to_all(parts[0], "y", 0, 0, tiled=True).sum(axis=0)
    early1 = lax.ppermute(early[j:], ROUND, AHEAD)
    across = lax.ppermute(jnp.stack([early[:j], early1]), "zh", SWAP)
    late = lax.all_to_all(parts[1], "y", 0, 0, tiled=True).sum(axis=0)
    late1 = lax.ppermute(late[j:], ROUND, AHEAD)
    return jnp.stack([late[:j], late1]) + across


def solution(mesh):
    split = Mesh(mesh.devices.reshape(SIZES), AXES)
    blk, col = ("zl", "x"), ("y", "zh", "core")
    return jax.shard_map(
        shards,
        mesh=split,
        in_specs=(P(col, blk), P(col, blk), P(col), P(col)),
        out_specs=P(None, None, AXES),
        check_vma=False,
    )
```

```python
import jax
import jax.numpy as jnp
from jax import lax
from jax.experimental import pallas as pl
from jax.experimental.pallas import tpu as pltpu
from jax.sharding import Mesh, PartitionSpec as P

AXES = ("zl", "x", "y", "zh", "core")
SIZES = (8, 4, 4, 2, 2)
NBLK = 32
LIMIT = pltpu.CompilerParams(vmem_limit_bytes=8 * 1024 * 1024)
SMEM = pl.BlockSpec(memory_space=pltpu.SMEM)
VMEM = pl.BlockSpec(memory_space=pltpu.VMEM)
ANY = pl.BlockSpec(memory_space=pl.ANY)


def on_chip(value):
    return pltpu.with_memory_space_constraint(value, pltpu.VMEM)


def dot(a, b, contract):
    return lax.dot_general(
        a, b, (contract, ((), ())), precision=lax.Precision.HIGHEST, preferred_element_type=jnp.float32
    )


def deflate_kernel(kept_ref, order_ref, merge_ref, ut_ref):
    n = merge_ref.shape[1]
    rows = lax.broadcasted_iota(jnp.int32, (n, n), 0)
    place = lax.broadcasted_iota(jnp.int32, (n, n), 1)
    hit = (rows == order_ref[...]) & (place < kept_ref[0])
    ut_ref[...] = dot(merge_ref[...], hit.astype(jnp.float32), ((1,), (0,)))


def deflate(kept, order, merge_t):
    return pl.pallas_call(
        deflate_kernel,
        out_shape=pltpu.VMEM(merge_t.shape, jnp.float32),
        in_specs=[SMEM, VMEM, VMEM],
        out_specs=VMEM,
        compiler_params=LIMIT,
        name="deflate",
    )(kept, order, merge_t)


def divide_kernel(core_ref, q_ref, send_ref, keep_ref, sem):
    pieces, _, width = send_ref.shape
    copies = []
    for side, target in ((1 - core_ref[0], send_ref), (core_ref[0], keep_ref)):
        for g in range(pieces):
            start = pl.multiple_of((2 * g + side) * width, width)
            copies.append(
                pltpu.make_async_copy(q_ref.at[:, pl.ds(start, width)], target.at[g], sem.at[len(copies)])
            )
    for c in copies:
        c.start()
    for c in copies:
        c.wait()


def divide(core, q, pieces):
    half = pltpu.VMEM((pieces, q.shape[0], q.shape[1] // (2 * pieces)), jnp.float32)
    return pl.pallas_call(
        divide_kernel,
        out_shape=(half, half),
        in_specs=[SMEM, ANY],
        out_specs=(VMEM, VMEM),
        scratch_shapes=[pltpu.SemaphoreType.DMA((2 * pieces,))],
        compiler_params=LIMIT,
        name="divide",
    )(core, q)


def multiply_kernel(where_ref, ut_ref, next_ref, keep_ref, got_ref, early_ref, late_ref):
    core, zh, flip = where_ref[0], where_ref[1], where_ref[2]
    j = ut_ref.shape[1]
    mine = jnp.concatenate([ut_ref[core], next_ref[core]], axis=0)
    theirs = jnp.concatenate([ut_ref[1 - core], next_ref[1 - core]], axis=0)
    u = jnp.concatenate([mine, theirs], axis=1)

    def block(g):
        return dot(u, jnp.concatenate([keep_ref[g], got_ref[g]], axis=0), ((1,), (0,)))

    for y in range(early_ref.shape[0]):
        first, second = block(2 * y + 1 - zh), block(2 * y + zh)
        early_ref[y, :j] = first[:j]
        late_ref[y, :j] = second[:j]
        early_ref[y, j:] = jnp.where(flip == 1, second[j:], first[j:])
        late_ref[y, j:] = jnp.where(flip == 1, first[j:], second[j:])


def multiply(where, ut, ut_next, keep, got):
    pieces, _, width = keep.shape
    out = pltpu.VMEM((pieces // 2, 2 * ut.shape[1], width), jnp.float32)
    return pl.pallas_call(
        multiply_kernel,
        out_shape=(out, out),
        in_specs=[SMEM, VMEM, VMEM, VMEM, VMEM],
        out_specs=(VMEM, VMEM),
        compiler_params=LIMIT,
        name="multiply",
    )(where, ut, ut_next, keep, got)


def pairs_of(move):
    pairs = []
    for b in range(NBLK):
        for zh in range(2):
            tb, tz = move(b, zh)
            pairs.append((b * 2 + zh, tb * 2 + tz))
    return pairs


BACK = pairs_of(lambda b, zh: ((b - 1) % NBLK, zh))
AHEAD = pairs_of(lambda b, zh: ((b + 1) % NBLK, zh if b < NBLK - 1 else 1 - zh))
SWAP = [(0, 1), (1, 0)]
ROUND = ("zl", "x", "zh")


def shards(old_vectors, merge_matrix, deflation_order, kept_counts):
    core = lax.axis_index("core").astype(jnp.int32)
    zh = lax.axis_index("zh").astype(jnp.int32)
    last = (lax.axis_index(("zl", "x")) == NBLK - 1).astype(jnp.int32)
    k, j = merge_matrix.shape
    ut = deflate(kept_counts, deflation_order.reshape(1, k), merge_matrix.T)
    ut = lax.all_gather(ut, "core")
    ut_next = lax.ppermute(ut, ROUND, BACK)
    send, keep = divide(core.reshape(1), old_vectors, 8)
    got = lax.ppermute(send, "core", SWAP)
    early, late = multiply(jnp.stack([core, zh, last]), ut, ut_next, keep, got)
    early = lax.all_to_all(early, "y", 0, 0, tiled=True)
    early1 = lax.ppermute(early[:, j:].sum(axis=0), ROUND, AHEAD)
    early0 = early[:, :j].sum(axis=0)
    mixed = jnp.stack([early0, early1])
    across = lax.ppermute(mixed, "zh", SWAP)
    late, _ = lax.optimization_barrier((late, mixed))
    late = lax.all_to_all(late, "y", 0, 0, tiled=True)
    late1 = lax.ppermute(late[:, j:].sum(axis=0), ROUND, AHEAD)
    late0 = late[:, :j].sum(axis=0)
    return jnp.stack([late0, late1]) + across


def solution(mesh):
    split = Mesh(mesh.devices.reshape(SIZES), AXES)
    blk, col = ("zl", "x"), ("y", "zh", "core")
    return jax.shard_map(
        shards,
        mesh=split,
        in_specs=(P(col, blk), P(col, blk), P(col), P(col)),
        out_specs=P(None, None, AXES),
        check_vma=False,
    )
```

```python
import jax
import jax.numpy as jnp
from jax import lax
from jax.experimental import pallas as pl
from jax.experimental.pallas import tpu as pltpu
from jax.sharding import Mesh, PartitionSpec as P


AXES = ("zl", "x", "y", "zh", "core")
SIZES = (8, 4, 4, 2, 2)
NBLK = 32
LIMIT = pltpu.CompilerParams(vmem_limit_bytes=8 * 1024 * 1024)
SMEM = pl.BlockSpec(memory_space=pltpu.SMEM)
VMEM = pl.BlockSpec(memory_space=pltpu.VMEM)
ANY = pl.BlockSpec(memory_space=pl.ANY)


def in_hbm(value):
    return pltpu.with_memory_space_constraint(value, pltpu.HBM)


def divide_kernel(core_ref, q_ref, send_ref, keep_ref, sem):
    pieces, _, width = send_ref.shape
    copies = []
    for side, target in ((1 - core_ref[0], send_ref), (core_ref[0], keep_ref)):
        for g in range(pieces):
            start = pl.multiple_of((2 * g + side) * width, width)
            copies.append(
                pltpu.make_async_copy(q_ref.at[:, pl.ds(start, width)], target.at[g], sem.at[len(copies)])
            )
    for c in copies:
        c.start()
    for c in copies:
        c.wait()


def divide(core, q, pieces):
    half = pltpu.VMEM((pieces, q.shape[0], q.shape[1] // (2 * pieces)), jnp.float32)
    return pl.pallas_call(
        divide_kernel,
        out_shape=(half, half),
        in_specs=[SMEM, ANY],
        out_specs=(VMEM, VMEM),
        scratch_shapes=[pltpu.SemaphoreType.DMA((2 * pieces,))],
        compiler_params=LIMIT,
        name="divide",
    )(core, in_hbm(q))


def deflate_kernel(kept_ref, order_ref, here_ref, next_ref, out_ref):
    _, n = here_ref.shape
    rows = lax.broadcasted_iota(jnp.int32, (n, n), 0)
    place = lax.broadcasted_iota(jnp.int32, (n, n), 1)
    hit = (rows == order_ref[...]) & (place < kept_ref[0])
    out_ref[...] = lax.dot_general(
        jnp.concatenate([here_ref[...], next_ref[...]], axis=0),
        hit.astype(jnp.float32),
        (((1,), (0,)), ((), ())),
        precision=lax.Precision.HIGHEST,
        preferred_element_type=jnp.float32,
    )


def deflate(kept, order, here, following):
    j, n = here.shape
    return pl.pallas_call(
        deflate_kernel,
        out_shape=pltpu.VMEM((2 * j, n), jnp.float32),
        in_specs=[SMEM, VMEM, VMEM, VMEM],
        out_specs=VMEM,
        compiler_params=LIMIT,
        name="deflate",
    )(kept, order, here, following)


def split(value):
    high = value.astype(jnp.bfloat16)
    low = (value - high.astype(jnp.float32)).astype(jnp.bfloat16)
    return high, low


def left_operand(u):
    high, low = split(u)
    return jnp.concatenate(
        [jnp.concatenate([high, high], axis=1), jnp.concatenate([low, jnp.zeros_like(low)], axis=1)], axis=0
    )


def right_operand(keep, got):
    kh, kl = split(keep)
    gh, gl = split(got)
    return jnp.concatenate([kh, gh, kl, gl], axis=0)


def product(left, right):
    both = lax.dot_general(left, right, (((1,), (0,)), ((), ())), preferred_element_type=jnp.float32)
    rows = left.shape[0] // 2
    return both[:rows] + both[rows:]


def first_kernel(where_ref, ut_ref, keep_ref, got_ref, out_ref):
    core, zh = where_ref[0], where_ref[1]
    u = jnp.concatenate([ut_ref[core], ut_ref[1 - core]], axis=1)
    j = u.shape[0] // 2
    both, last = left_operand(u), left_operand(u[j:])
    for y in range(out_ref.shape[0]):
        far, near = 2 * y + 1 - zh, 2 * y + zh
        out_ref[y, : 2 * j] = product(both, right_operand(keep_ref[far], got_ref[far]))
        out_ref[y, 2 * j :] = product(last, right_operand(keep_ref[near], got_ref[near]))


def second_kernel(where_ref, ut_ref, keep_ref, got_ref, out_ref):
    core, zh = where_ref[0], where_ref[1]
    u = jnp.concatenate([ut_ref[core], ut_ref[1 - core]], axis=1)
    left = left_operand(u[: u.shape[0] // 2])
    for y in range(out_ref.shape[0]):
        near = 2 * y + zh
        out_ref[y] = product(left, right_operand(keep_ref[near], got_ref[near]))


def multiply(kernel, rows, where, ut, keep, got):
    pieces, _, width = keep.shape
    return pl.pallas_call(
        kernel,
        out_shape=pltpu.VMEM((pieces // 2, rows, width), jnp.float32),
        in_specs=[SMEM, VMEM, VMEM, VMEM],
        out_specs=VMEM,
        compiler_params=LIMIT,
    )(where, ut, keep, got)


def pairs_of(blocks, move):
    pairs = []
    for b in blocks:
        for zh in range(2):
            tb, tz = move(b, zh)
            pairs.append((b * 2 + zh, tb * 2 + tz))
    return pairs


LAST = NBLK - 1
BACK = pairs_of(range(NBLK), lambda b, zh: ((b - 1) % NBLK, zh))
AHEAD = pairs_of(range(LAST), lambda b, zh: (b + 1, zh))
WRAP_SAME = pairs_of([LAST], lambda b, zh: (0, zh))
WRAP_OTHER = pairs_of([LAST], lambda b, zh: (0, 1 - zh))
SWAP = [(0, 1), (1, 0)]
ROUND = ("zl", "x", "zh")


def over_y(value):
    return lax.all_to_all(value, "y", 0, 0, tiled=True)


def shards(old_vectors, merge_matrix, deflation_order, kept_counts):
    core = lax.axis_index("core").astype(jnp.int32)
    zh = lax.axis_index("zh").astype(jnp.int32)
    where = jnp.stack([core, zh])
    k, j = merge_matrix.shape
    merge_t = merge_matrix.T
    following = lax.ppermute(merge_t, ROUND, BACK)
    send, keep = divide(core.reshape(1), old_vectors, 8)
    got = lax.ppermute(send, "core", SWAP)
    ut = deflate(kept_counts, deflation_order.reshape(1, k), merge_t, following)
    ut = lax.all_gather(ut, "core")
    first = multiply(first_kernel, 3 * j, where, ut, keep, got)
    first = over_y(first)
    keep = lax.optimization_barrier((keep, first))[0]
    sum1 = first[:, j:].sum(axis=0)
    moved = lax.ppermute(sum1, ROUND, AHEAD)
    other = lax.ppermute(sum1[:j], ROUND, WRAP_OTHER)
    same = lax.ppermute(sum1[j:], ROUND, WRAP_SAME)
    sum0 = first[:, :j].sum(axis=0)
    across = lax.ppermute(jnp.concatenate([sum0, moved[:j]], axis=0), "zh", SWAP)
    second = multiply(second_kernel, j, where, ut, keep, got)
    second = over_y(second)
    second, moved, same, other, across = lax.optimization_barrier((second, moved, same, other, across))
    own = jnp.concatenate([second.sum(axis=0), moved[j:] + same + other], axis=0)
    return (own + across).reshape(2, j, -1)


def solution(mesh):
    split = Mesh(mesh.devices.reshape(SIZES), AXES)
    blk, col = ("zl", "x"), ("y", "zh", "core")
    return jax.shard_map(
        shards,
        mesh=split,
        in_specs=(P(col, blk), P(col, blk), P(col), P(col)),
        out_specs=P(None, None, AXES),
        check_vma=False,
    )
```

```python
import jax
import jax.numpy as jnp
from jax import lax
from jax.experimental import pallas as pl
from jax.experimental.pallas import tpu as pltpu
from jax.sharding import Mesh, PartitionSpec as P


AXES = ("zl", "x", "y", "zh", "core")
SIZES = (8, 4, 4, 2, 2)
NBLK = 32
LIMIT = pltpu.CompilerParams(vmem_limit_bytes=8 * 1024 * 1024)
SMEM = pl.BlockSpec(memory_space=pltpu.SMEM)
VMEM = pl.BlockSpec(memory_space=pltpu.VMEM)
ANY = pl.BlockSpec(memory_space=pl.ANY)


def in_hbm(value):
    return pltpu.with_memory_space_constraint(value, pltpu.HBM)


def divide_kernel(core_ref, q_ref, send_ref, keep_ref, sem):
    pieces, _, width = send_ref.shape
    copies = []
    for side, target in ((1 - core_ref[0], send_ref), (core_ref[0], keep_ref)):
        for g in range(pieces):
            start = pl.multiple_of((2 * g + side) * width, width)
            copies.append(
                pltpu.make_async_copy(q_ref.at[:, pl.ds(start, width)], target.at[g], sem.at[len(copies)])
            )
    for c in copies:
        c.start()
    for c in copies:
        c.wait()


def divide(core, q, pieces):
    half = pltpu.VMEM((pieces, q.shape[0], q.shape[1] // (2 * pieces)), jnp.float32)
    return pl.pallas_call(
        divide_kernel,
        out_shape=(half, half),
        in_specs=[SMEM, ANY],
        out_specs=(VMEM, VMEM),
        scratch_shapes=[pltpu.SemaphoreType.DMA((2 * pieces,))],
        compiler_params=LIMIT,
        name="divide",
    )(core, in_hbm(q))


def deflate_kernel(kept_ref, order_ref, here_ref, next_ref, out_ref):
    _, n = here_ref.shape
    rows = lax.broadcasted_iota(jnp.int32, (n, n), 0)
    place = lax.broadcasted_iota(jnp.int32, (n, n), 1)
    hit = (rows == order_ref[...]) & (place < kept_ref[0])
    out_ref[...] = lax.dot_general(
        jnp.concatenate([here_ref[...], next_ref[...]], axis=0),
        hit.astype(jnp.float32),
        (((1,), (0,)), ((), ())),
        precision=lax.Precision.HIGHEST,
        preferred_element_type=jnp.float32,
    )


def deflate(kept, order, here, following):
    j, n = here.shape
    return pl.pallas_call(
        deflate_kernel,
        out_shape=pltpu.VMEM((2 * j, n), jnp.float32),
        in_specs=[SMEM, VMEM, VMEM, VMEM],
        out_specs=VMEM,
        compiler_params=LIMIT,
        name="deflate",
    )(kept, order, here, following)


def split(value):
    high = value.astype(jnp.bfloat16)
    low = (value - high.astype(jnp.float32)).astype(jnp.bfloat16)
    return high, low


def left_operand(u):
    high, low = split(u)
    return jnp.concatenate(
        [jnp.concatenate([high, high], axis=1), jnp.concatenate([low, jnp.zeros_like(low)], axis=1)], axis=0
    )


def right_operand(keep, got):
    kh, kl = split(keep)
    gh, gl = split(got)
    return jnp.concatenate([kh, gh, kl, gl], axis=0)


def product(left, right):
    both = lax.dot_general(left, right, (((1,), (0,)), ((), ())), preferred_element_type=jnp.float32)
    rows = left.shape[0] // 2
    return both[:rows] + both[rows:]


def first_kernel(where_ref, ut_ref, keep_ref, got_ref, out_ref):
    core, zh = where_ref[0], where_ref[1]
    u = jnp.concatenate([ut_ref[core], ut_ref[1 - core]], axis=1)
    j = u.shape[0] // 2
    both, last = left_operand(u), left_operand(u[j:])
    for y in range(out_ref.shape[0]):
        far, near = 2 * y + 1 - zh, 2 * y + zh
        out_ref[y, : 2 * j] = product(both, right_operand(keep_ref[far], got_ref[far]))
        out_ref[y, 2 * j :] = product(last, right_operand(keep_ref[near], got_ref[near]))


def second_kernel(where_ref, ut_ref, keep_ref, got_ref, out_ref):
    core, zh = where_ref[0], where_ref[1]
    u = jnp.concatenate([ut_ref[core], ut_ref[1 - core]], axis=1)
    left = left_operand(u[: u.shape[0] // 2])
    for y in range(out_ref.shape[0]):
        near = 2 * y + zh
        out_ref[y] = product(left, right_operand(keep_ref[near], got_ref[near]))


def multiply(kernel, rows, where, ut, keep, got):
    pieces, _, width = keep.shape
    return pl.pallas_call(
        kernel,
        out_shape=pltpu.VMEM((pieces // 2, rows, width), jnp.float32),
        in_specs=[SMEM, VMEM, VMEM, VMEM],
        out_specs=VMEM,
        compiler_params=LIMIT,
    )(where, ut, keep, got)


def pairs_of(blocks, move):
    pairs = []
    for b in blocks:
        for zh in range(2):
            tb, tz = move(b, zh)
            pairs.append((b * 2 + zh, tb * 2 + tz))
    return pairs


LAST = NBLK - 1
BACK = pairs_of(range(NBLK), lambda b, zh: ((b - 1) % NBLK, zh))
AHEAD = pairs_of(range(1, LAST), lambda b, zh: (b + 1, zh))
WRAP_SAME = pairs_of([LAST, 0], lambda b, zh: ((b + 1) % NBLK, zh))
WRAP_OTHER = pairs_of([LAST], lambda b, zh: (0, 1 - zh)) + pairs_of([0], lambda b, zh: (1, 1 - zh))[1:]
NEXT_OTHER = pairs_of([0], lambda b, zh: (1, 1 - zh))[:1]
SWAP = [(0, 1), (1, 0)]
ROUND = ("zl", "x", "zh")


def over_y(value):
    return lax.all_to_all(value, "y", 0, 0, tiled=True)


def shards(old_vectors, merge_matrix, deflation_order, kept_counts):
    core = lax.axis_index("core").astype(jnp.int32)
    zh = lax.axis_index("zh").astype(jnp.int32)
    where = jnp.stack([core, zh])
    k, j = merge_matrix.shape
    merge_t = merge_matrix.T
    following = lax.ppermute(merge_t, ROUND, BACK)
    send, keep = divide(core.reshape(1), old_vectors, 8)
    got = lax.ppermute(send, "core", SWAP)
    ut = deflate(kept_counts, deflation_order.reshape(1, k), merge_t, following)
    ut = lax.all_gather(ut, "core")
    first = multiply(first_kernel, 3 * j, where, ut, keep, got)
    first = over_y(first)
    keep = lax.optimization_barrier((keep, first))[0]
    sum1 = first[:, j:].sum(axis=0)
    moved = lax.ppermute(sum1, ROUND, AHEAD)
    other = lax.ppermute(sum1[:j], ROUND, WRAP_OTHER)
    same = lax.ppermute(sum1[j:], ROUND, WRAP_SAME)
    sum0 = first[:, :j].sum(axis=0)
    across = lax.ppermute(jnp.concatenate([sum0, moved[:j]], axis=0), "zh", SWAP)
    beyond = lax.ppermute(sum1[:j], ROUND, NEXT_OTHER)
    second = multiply(second_kernel, j, where, ut, keep, got)
    second = over_y(second)
    second, moved, same, other, beyond, across = lax.optimization_barrier((second, moved, same, other, beyond, across))
    own = jnp.concatenate([second.sum(axis=0), moved[j:] + same + other + beyond], axis=0)
    return (own + across).reshape(2, j, -1)


def solution(mesh):
    split = Mesh(mesh.devices.reshape(SIZES), AXES)
    blk, col = ("zl", "x"), ("y", "zh", "core")
    return jax.shard_map(
        shards,
        mesh=split,
        in_specs=(P(col, blk), P(col, blk), P(col), P(col)),
        out_specs=P(None, None, AXES),
        check_vma=False,
    )
```

```python
import jax
import jax.numpy as jnp
from jax import lax
from jax.experimental import pallas as pl
from jax.experimental.pallas import tpu as pltpu
from jax.sharding import Mesh, PartitionSpec as P


AXES = ("zl", "x", "y", "zh", "core")
SIZES = (8, 4, 4, 2, 2)
NBLK = 32
LIMIT = pltpu.CompilerParams(vmem_limit_bytes=8 * 1024 * 1024)
SMEM = pl.BlockSpec(memory_space=pltpu.SMEM)
VMEM = pl.BlockSpec(memory_space=pltpu.VMEM)
ANY = pl.BlockSpec(memory_space=pl.ANY)


def in_hbm(value):
    return pltpu.with_memory_space_constraint(value, pltpu.HBM)


def divide_kernel(core_ref, q_ref, send_ref, keep_ref, sem):
    pieces, _, width = send_ref.shape
    copies = []
    for side, target in ((1 - core_ref[0], send_ref), (core_ref[0], keep_ref)):
        for g in range(pieces):
            start = pl.multiple_of((2 * g + side) * width, width)
            copies.append(
                pltpu.make_async_copy(q_ref.at[:, pl.ds(start, width)], target.at[g], sem.at[len(copies)])
            )
    for c in copies:
        c.start()
    for c in copies:
        c.wait()


def divide(core, q, pieces):
    half = pltpu.VMEM((pieces, q.shape[0], q.shape[1] // (2 * pieces)), jnp.float32)
    return pl.pallas_call(
        divide_kernel,
        out_shape=(half, half),
        in_specs=[SMEM, ANY],
        out_specs=(VMEM, VMEM),
        scratch_shapes=[pltpu.SemaphoreType.DMA((2 * pieces,))],
        compiler_params=LIMIT,
        name="divide",
    )(core, in_hbm(q))


def deflate_kernel(kept_ref, order_ref, here_ref, next_ref, out_ref):
    _, n = here_ref.shape
    rows = lax.broadcasted_iota(jnp.int32, (n, n), 0)
    place = lax.broadcasted_iota(jnp.int32, (n, n), 1)
    hit = (rows == order_ref[...]) & (place < kept_ref[0])
    out_ref[...] = lax.dot_general(
        jnp.concatenate([here_ref[...], next_ref[...]], axis=0),
        hit.astype(jnp.float32),
        (((1,), (0,)), ((), ())),
        precision=lax.Precision.HIGHEST,
        preferred_element_type=jnp.float32,
    )


def deflate(kept, order, here, following):
    j, n = here.shape
    return pl.pallas_call(
        deflate_kernel,
        out_shape=pltpu.VMEM((2 * j, n), jnp.float32),
        in_specs=[SMEM, VMEM, VMEM, VMEM],
        out_specs=VMEM,
        compiler_params=LIMIT,
        name="deflate",
    )(kept, order, here, following)


def split(value):
    high = value.astype(jnp.bfloat16)
    low = (value - high.astype(jnp.float32)).astype(jnp.bfloat16)
    return high, low


def left_operand(u):
    high, low = split(u)
    return jnp.concatenate(
        [jnp.concatenate([high, high], axis=1), jnp.concatenate([low, jnp.zeros_like(low)], axis=1)], axis=0
    )


def right_operand(keep, got):
    kh, kl = split(keep)
    gh, gl = split(got)
    return jnp.concatenate([kh, gh, kl, gl], axis=0)


def product(left, right):
    both = lax.dot_general(left, right, (((1,), (0,)), ((), ())), preferred_element_type=jnp.float32)
    rows = left.shape[0] // 2
    return both[:rows] + both[rows:]


def first_kernel(where_ref, ut_ref, keep_ref, got_ref, out_ref):
    core, zh = where_ref[0], where_ref[1]
    u = jnp.concatenate([ut_ref[core], ut_ref[1 - core]], axis=1)
    j = u.shape[0] // 2
    both, last = left_operand(u), left_operand(u[j:])
    for y in range(out_ref.shape[0]):
        far, near = 2 * y + 1 - zh, 2 * y + zh
        out_ref[y, : 2 * j] = product(both, right_operand(keep_ref[far], got_ref[far]))
        out_ref[y, 2 * j :] = product(last, right_operand(keep_ref[near], got_ref[near]))


def second_kernel(where_ref, ut_ref, keep_ref, got_ref, out_ref):
    core, zh = where_ref[0], where_ref[1]
    u = jnp.concatenate([ut_ref[core], ut_ref[1 - core]], axis=1)
    left = left_operand(u[: u.shape[0] // 2])
    for y in range(out_ref.shape[0]):
        near = 2 * y + zh
        out_ref[y] = product(left, right_operand(keep_ref[near], got_ref[near]))


def multiply(kernel, rows, where, ut, keep, got):
    pieces, _, width = keep.shape
    return pl.pallas_call(
        kernel,
        out_shape=pltpu.VMEM((pieces // 2, rows, width), jnp.float32),
        in_specs=[SMEM, VMEM, VMEM, VMEM],
        out_specs=VMEM,
        compiler_params=LIMIT,
    )(where, ut, keep, got)


def join_kernel(top_ref, moved_ref, out_ref):
    j = top_ref.shape[0]
    out_ref[:j] = top_ref[...]
    out_ref[j:] = moved_ref[:j]


def join(top, moved):
    return pl.pallas_call(
        join_kernel,
        out_shape=pltpu.VMEM(moved.shape, jnp.float32),
        in_specs=[VMEM, VMEM],
        out_specs=VMEM,
        compiler_params=LIMIT,
        name="join",
    )(top, moved)


def pairs_of(blocks, move):
    pairs = []
    for b in blocks:
        for zh in range(2):
            tb, tz = move(b, zh)
            pairs.append((b * 2 + zh, tb * 2 + tz))
    return pairs


LAST = NBLK - 1
BACK = pairs_of(range(NBLK), lambda b, zh: ((b - 1) % NBLK, zh))
AHEAD = pairs_of(range(1, LAST), lambda b, zh: (b + 1, zh))
WRAP_SAME = pairs_of([LAST, 0], lambda b, zh: ((b + 1) % NBLK, zh))
WRAP_OTHER = pairs_of([LAST], lambda b, zh: (0, 1 - zh)) + pairs_of([0], lambda b, zh: (1, 1 - zh))[1:]
NEXT_OTHER = pairs_of([0], lambda b, zh: (1, 1 - zh))[:1]
SWAP = [(0, 1), (1, 0)]
ROUND = ("zl", "x", "zh")


def over_y(value):
    return lax.all_to_all(value, "y", 0, 0, tiled=True)


def shards(old_vectors, merge_matrix, deflation_order, kept_counts):
    core = lax.axis_index("core").astype(jnp.int32)
    zh = lax.axis_index("zh").astype(jnp.int32)
    where = jnp.stack([core, zh])
    k, j = merge_matrix.shape
    merge_t = merge_matrix.T
    following = lax.ppermute(merge_t, ROUND, BACK)
    send, keep = divide(core.reshape(1), old_vectors, 8)
    got = lax.ppermute(send, "core", SWAP)
    ut = deflate(kept_counts, deflation_order.reshape(1, k), merge_t, following)
    ut = lax.all_gather(ut, "core")
    first = multiply(first_kernel, 3 * j, where, ut, keep, got)
    first = over_y(first)
    keep = lax.optimization_barrier((keep, first))[0]
    sum1 = first[:, j:].sum(axis=0)
    moved = lax.ppermute(sum1, ROUND, AHEAD)
    other = lax.ppermute(sum1[:j], ROUND, WRAP_OTHER)
    same = lax.ppermute(sum1[j:], ROUND, WRAP_SAME)
    sum0 = first[:, :j].sum(axis=0)
    across = lax.ppermute(join(sum0, moved), "zh", SWAP)
    beyond = lax.ppermute(sum1[:j], ROUND, NEXT_OTHER)
    second = multiply(second_kernel, j, where, ut, keep, got)
    second = over_y(second)
    second, moved, same, other, beyond, across = lax.optimization_barrier(
        (second, moved, same, other, beyond, across)
    )
    own = jnp.concatenate([second.sum(axis=0), moved[j:] + same + other + beyond], axis=0)
    return (own + across).reshape(2, j, -1)


def solution(mesh):
    split = Mesh(mesh.devices.reshape(SIZES), AXES)
    blk, col = ("zl", "x"), ("y", "zh", "core")
    return jax.shard_map(
        shards,
        mesh=split,
        in_specs=(P(col, blk), P(col, blk), P(col), P(col)),
        out_specs=P(None, None, AXES),
        check_vma=False,
    )
```
